32 devices in a mesh: inst: 4 (over y, x), head: 8 (over z, core).
Axes of the slice: x: 2, y: 2, z: 4, core: 2. Of those that a mesh axis runs over, the one named last changes fastest.
Arguments:
- old_keys: bfloat16 [512, 16, 64, 128], P('inst', 'head'), may hold values from -6 to 6
- old_values: bfloat16 [512, 16, 64, 128], P('inst', 'head'), may hold values from -6 to 6
- old_block: int32 [512], P('inst'), may hold values from -1 to 127, as said below
- new_slot: int32 [128], replicated, may hold values from 0 to 127, as said below
- lengths: int32 [64], replicated, may hold values from 1 to 8192, as said below
- queries: bfloat16 [64, 16, 8192], P(None, None, 'head'), may hold values from -240 to 240
- draft_keys: bfloat16 [64, 16, 1024], P('inst'), may hold values from -6 to 6
- draft_values: bfloat16 [64, 16, 1024], P('inst'), may hold values from -6 to 6
Outputs:
- moved_keys: bfloat16 [128, 16, 64, 128], P('inst', 'head')
- moved_values: bfloat16 [128, 16, 64, 128], P('inst', 'head')
- attended: bfloat16 [64, 16, 8192], P(None, None, 'head')
The draws below stay inside these ranges and needn't reach their ends.
Inputs may be any that keep to these rules, and one draw needn't show every extreme that they name: ceil(lengths / 128) summed over the requests is exactly 128; the longest request has exactly 8192 tokens. `old_block`: every block 0 to 127 stands in exactly one old slot; the blocks fill all slots of 1 instances and all other slots hold -1. A permutation; block g goes to instance new_slot[g] // 32. At most 32 blocks go from one old instance to one new one, and in every draw some new instance receives all its 32 blocks from a single old instance.
All inputs are finite; a program needn't handle non-finite values.
Results may differ from the reference program's by a relative error of at most 0.004.
Values may be sent and summed in bfloat16 or wider, within the bound.
A program may use at most 64 MiB of HBM per device.

```python
import math
import jax
import jax.numpy as jnp
from jax import lax

KVH = 8
HD = 128
GROUP = 8
BLK = 128
REQ = 64
DRAFT = 16
BLOCKS_PER_RANK = 32
QH = 64
HALF = 64
OLD_INST = 1
SLOTS = 128
TOTAL_BLOCKS = 128
MAX_BLOCKS = 64
N_INST = 4


def build_tables(key):
    base = jax.random.fold_in(key, 11)
    key_old, key_shuffle, foreign_key_rows, key_owners = jax.random.split(base, 4)
    chosen = jnp.sort(jax.random.permutation(key_old, N_INST)[:OLD_INST]).astype(jnp.int32)
    shuffle = jax.random.permutation(key_shuffle, TOTAL_BLOCKS).astype(jnp.int32)
    places = jnp.arange(TOTAL_BLOCKS, dtype=jnp.int32)
    old_position = chosen[places // SLOTS] * SLOTS + places % SLOTS
    old_table = jnp.full((N_INST * SLOTS,), -1, jnp.int32).at[old_position].set(shuffle)
    peer_replicas = (BLOCKS_PER_RANK + jax.random.permutation(foreign_key_rows, TOTAL_BLOCKS - BLOCKS_PER_RANK)).astype(jnp.int32)
    token_position = jnp.concatenate([jnp.arange(BLOCKS_PER_RANK, dtype=jnp.int32), peer_replicas])
    block_owner_list = jax.random.permutation(key_owners, N_INST).astype(jnp.int32)
    destination_replica = block_owner_list[token_position // BLOCKS_PER_RANK] * BLOCKS_PER_RANK + token_position % BLOCKS_PER_RANK
    new_table = jnp.zeros((TOTAL_BLOCKS,), jnp.int32).at[shuffle].set(destination_replica)
    return (old_table, new_table)


def draw_old_block(key, part):
    return build_tables(key)[0]


def draw_new_slot(key, part):
    return build_tables(key)[1]


def draw_lengths(key, part):
    base = jax.random.fold_in(key, 23)
    key_long, key_weight, key_fill = jax.random.split(base, 3)
    longest = jax.random.randint(key_long, (), 0, REQ)
    request_ids = jnp.arange(REQ, dtype=jnp.int32)
    peer_replicas = request_ids != longest
    weights = jnp.where(peer_replicas, jax.random.randint(key_weight, (REQ,), 1, 5), 0).astype(jnp.int32)
    weight_sum = jnp.sum(weights)
    excess = TOTAL_BLOCKS - MAX_BLOCKS - (REQ - 1)
    shares = excess * weights // weight_sum
    leftover = excess - jnp.sum(shares)
    ranking = jnp.cumsum(peer_replicas.astype(jnp.int32)) - 1
    counts = jnp.where(peer_replicas, 1 + shares + (ranking < leftover).astype(jnp.int32), MAX_BLOCKS)
    filling = jnp.where(peer_replicas, jax.random.randint(key_fill, (REQ,), 1, BLK + 1), BLK)
    return ((counts - 1) * BLK + filling).astype(jnp.int32)


def draw_queries(key, part):
    base = jax.random.fold_in(key, 37)
    key_value, key_scale = jax.random.split(base)
    entries_drawn = jax.random.normal(key_value, (REQ, DRAFT, QH, HD), jnp.float32)
    scales = jnp.exp(jax.random.uniform(key_scale, (REQ, 1, QH, 1), jnp.float32, math.log(1.0), math.log(6.0)))
    return jnp.clip(entries_drawn * scales, -240.0, 240.0).reshape(REQ, DRAFT, QH * HD).astype(jnp.bfloat16)


def block_levels(rng, dims, cuts, least, largest):
    level = 1.0
    for axis_at, blocks in cuts:
        heights = jax.random.uniform(jax.random.fold_in(jax.random.fold_in(rng, 6), axis_at), (blocks,), jnp.float32, least / len(cuts), largest / len(cuts))
        level = level * jnp.repeat(jnp.exp(heights), dims[axis_at] // blocks).reshape((-1,) + (1,) * (len(dims) - 1 - axis_at))
    return level


def noise(own_key, dims, spread, most, cuts=(), kind=jnp.bfloat16):
    entries = spread * jax.random.normal(own_key, dims, jnp.float32)
    if cuts:
        entries = entries * block_levels(own_key, dims, cuts, -0.22, 0.18)
    return jnp.clip(entries, -most, most).astype(kind)


def setup_inputs(seed: int = 0) -> dict:
    streams_of = jax.random.split(jax.random.key(seed), 9)
    old_keys = noise(streams_of[0], (N_INST * SLOTS, 2 * KVH, HALF, HD), 1.0, 6.0, ((0, 4), (1, 8)))
    old_values = noise(streams_of[1], (N_INST * SLOTS, 2 * KVH, HALF, HD), 1.0, 6.0, ((0, 4), (1, 8)))
    old_block = draw_old_block(jax.random.fold_in(streams_of[8], 71), 0)
    new_slot = draw_new_slot(jax.random.fold_in(streams_of[8], 71), 0)
    lengths = draw_lengths(jax.random.fold_in(streams_of[8], 71), 0)
    queries = draw_queries(jax.random.fold_in(streams_of[8], 71), 0)
    draft_keys = noise(streams_of[6], (REQ, DRAFT, KVH * HD), 1.0, 6.0, ((0, 4),))
    draft_values = noise(streams_of[7], (REQ, DRAFT, KVH * HD), 1.0, 6.0, ((0, 4),))
    return {"old_keys": old_keys, "old_values": old_values, "old_block": old_block, "new_slot": new_slot, "lengths": lengths, "queries": queries, "draft_keys": draft_keys, "draft_values": draft_values}


masked = -1e+30

def reference(old_keys, old_values, old_block, new_slot, lengths, queries, draft_keys, draft_values):
    slot_count = old_keys.shape[0]
    block_capacity = new_slot.shape[0]
    block_ids = jnp.arange(block_capacity, dtype=jnp.int32)
    holder = jnp.zeros((block_capacity,), jnp.int32).at[jnp.where(old_block >= 0, old_block, block_capacity)].set(jnp.arange(slot_count, dtype=jnp.int32), mode='drop')
    locally_present = jnp.zeros((block_capacity,), jnp.int32).at[new_slot].set(block_ids)
    source = holder[locally_present]
    moved_keys = old_keys[source]
    moved_values = old_values[source]
    inv_root = 1.0 / math.sqrt(HD)
    counts = (lengths + BLK - 1) // BLK
    starts = jnp.cumsum(counts) - counts
    block_owner_list = (lax.optimization_barrier(jnp.sum((starts[None, :] <= locally_present[:, None]).astype(jnp.int32), axis=1)) - 1).astype(jnp.int32)
    offset = locally_present - starts[block_owner_list]
    positions = offset[:, None] * BLK + jnp.arange(BLK, dtype=jnp.int32)[None, :]
    usable = positions < lengths[block_owner_list][:, None]
    qcount = DRAFT * GROUP
    split_q = queries.reshape(REQ, DRAFT, KVH, GROUP, HD)
    grouped = split_q.transpose(0, 2, 1, 3, 4).reshape(REQ, KVH, qcount, HD)
    dkeys = draft_keys.reshape(REQ, DRAFT, KVH, HD).astype(jnp.float32)
    dvals = draft_values.reshape(REQ, DRAFT, KVH, HD).astype(jnp.float32)
    dscore = jnp.einsum('rikgd,rjkd->rkigj', split_q.astype(jnp.float32), dkeys) * inv_root
    causal = jnp.arange(DRAFT)[None, :] <= jnp.arange(DRAFT)[:, None]
    causal_flat = jnp.broadcast_to(causal[:, None, :], (DRAFT, GROUP, DRAFT)).reshape(qcount, DRAFT)
    dscore = jnp.where(causal_flat, dscore.reshape(REQ, KVH, qcount, DRAFT), masked)
    stride = math.gcd(block_capacity, 64)
    nsteps = block_capacity // stride
    key_blocks = moved_keys.reshape(nsteps, stride, KVH, BLK, HD)
    value_blocks = moved_values.reshape(nsteps, stride, KVH, BLK, HD)
    owner_blocks = block_owner_list.reshape(nsteps, stride)
    usable_blocks = usable.reshape(nsteps, stride, BLK)
    request_ids = jnp.arange(REQ, dtype=jnp.int32)

    def scores_of(key_rows, rows_owner, rows_usable):
        picked = grouped[rows_owner].astype(jnp.float32)
        scores = jnp.einsum('skqd,sktd->skqt', picked, key_rows.astype(jnp.float32)) * inv_root
        return jnp.where(rows_usable[:, None, None, :], scores, masked)

    def first_pass(peaks, pieces):
        key_rows, rows_owner, rows_usable = pieces
        scores = scores_of(key_rows, rows_owner, rows_usable)
        belongs = rows_owner[:, None] == request_ids[None, :]
        slot_peaks = lax.optimization_barrier(jnp.max(scores, axis=-1))
        block_peak = lax.optimization_barrier(jnp.max(jnp.where(belongs[:, :, None, None], slot_peaks[:, None], masked), axis=0))
        return (jnp.maximum(peaks, block_peak), None)
    peaks = lax.scan(first_pass, lax.optimization_barrier(jnp.max(dscore, axis=-1)), (key_blocks, owner_blocks, usable_blocks))[0]

    def second_pass(state_now, pieces):
        totals, weighted = state_now
        key_rows, value_rows, rows_owner, rows_usable = pieces
        scores = scores_of(key_rows, rows_owner, rows_usable)
        weights = jnp.where(rows_usable[:, None, None, :], jnp.exp(scores - peaks[rows_owner][..., None]), 0.0)
        belongs = (rows_owner[:, None] == request_ids[None, :]).astype(jnp.float32)
        totals = totals + jnp.einsum('sr,skq->rkq', belongs, lax.optimization_barrier(jnp.sum(weights, axis=-1)), precision=lax.Precision.HIGHEST)
        rounded = weights.astype(jnp.bfloat16).astype(jnp.float32)
        blended = jnp.einsum('skqt,sktd->skqd', rounded, value_rows.astype(jnp.float32))
        weighted = weighted + jnp.einsum('sr,skqd->rkqd', belongs, blended, precision=lax.Precision.HIGHEST)
        return ((totals, weighted), None)
    start_state = (jnp.zeros((REQ, KVH, qcount), jnp.float32), jnp.zeros((REQ, KVH, qcount, HD), jnp.float32))
    totals, weighted = lax.scan(second_pass, start_state, (key_blocks, value_blocks, owner_blocks, usable_blocks))[0]
    dweights = jnp.where(causal_flat, jnp.exp(dscore - peaks[..., None]), 0.0)
    totals = totals + lax.optimization_barrier(jnp.sum(dweights, axis=-1))
    drounded = dweights.astype(jnp.bfloat16).astype(jnp.float32)
    weighted = weighted + jnp.einsum('rkqj,rjkd->rkqd', drounded, dvals)
    result = weighted / totals[..., None]
    result = result.reshape(REQ, KVH, DRAFT, GROUP, HD).transpose(0, 2, 1, 3, 4).reshape(REQ, DRAFT, QH * HD)
    return (moved_keys, moved_values, result.astype(jnp.bfloat16))
```

```python
import functools
import math

import jax
import jax.numpy as jnp
from jax import lax
from jax.experimental import pallas as pl
from jax.experimental.pallas import tpu as pltpu
from jax.sharding import PartitionSpec as P

GROUP = 8
BLK = 128
DRAFT = 16


masked = -1e30


def partner_2(block, axis, stride):
    count = lax.axis_size(axis)
    route = []
    for low in range(count):
        high = low | 1 << stride
        if high != low and high < count:
            route += [(low, high), (high, low)]
    return lax.ppermute(block, axis, route)


def join_partials(earlier, later):
    raised = jnp.maximum(earlier[0], later[0])
    keep_early = jnp.exp(earlier[0] - raised)
    keep_late = jnp.exp(later[0] - raised)
    totals = earlier[1] * keep_early + later[1] * keep_late
    weighted = earlier[2] * keep_early[..., None] + later[2] * keep_late[..., None]
    return (raised, totals, weighted)


def cache_partial(key_cache, value_cache, block_list, lengths, grouped, head_base):
    slot_count, entries, half_len, head_dim = key_cache.shape
    requests, qcount, _ = grouped.shape
    inv_root = 1.0 / math.sqrt(head_dim)
    counts = (lengths + BLK - 1) // BLK
    starts = jnp.cumsum(counts) - counts
    filled = block_list >= 0
    block_owner_list = (
        jnp.sum((starts[None, :] <= block_list[:, None]).astype(jnp.int32), axis=1) - 1
    )
    block_owner_list = jnp.clip(block_owner_list, 0, requests - 1)
    offset = block_list - starts[block_owner_list]
    halves = (head_base + jnp.arange(entries, dtype=jnp.int32)) % 2
    within = (halves[:, None] * half_len + jnp.arange(half_len, dtype=jnp.int32)[None, :]).reshape(
        entries * half_len
    )
    positions = offset[:, None] * BLK + within[None, :]
    usable = filled[:, None] & (positions < lengths[block_owner_list][:, None])
    stride = math.gcd(slot_count, 64)
    nsteps = slot_count // stride
    token_count = entries * half_len
    key_rows_all = key_cache.reshape(nsteps, stride, token_count, head_dim)
    value_rows_all = value_cache.reshape(nsteps, stride, token_count, head_dim)
    request_ids = jnp.arange(requests, dtype=jnp.int32)

    def advance(state_now, pieces):
        peaks, totals, weighted = state_now
        key_rows, value_rows, rows_owner, rows_filled, rows_usable = pieces
        picked = grouped[rows_owner]
        scores = (
            jnp.einsum("sqd,std->sqt", picked, key_rows, preferred_element_type=jnp.float32)
            * inv_root
        )
        scores = jnp.where(rows_usable[:, None, :], scores, masked)
        belongs = (rows_owner[:, None] == request_ids[None, :]) & rows_filled[:, None]
        slot_peaks = jnp.max(scores, axis=-1)
        block_peak = jnp.max(jnp.where(belongs[:, :, None], slot_peaks[:, None, :], masked), axis=0)
        raised = jnp.maximum(peaks, block_peak)
        weights = jnp.where(
            rows_usable[:, None, :], jnp.exp(scores - raised[rows_owner][:, :, None]), 0.0
        )
        belongs_f = belongs.astype(jnp.float32)
        row_sums = jnp.dot(
            belongs_f.T,
            jnp.sum(weights, axis=-1),
            precision=lax.Precision.HIGHEST,
            preferred_element_type=jnp.float32,
        )
        blended = jnp.einsum(
            "sqt,std->sqd",
            weights.astype(jnp.bfloat16),
            value_rows,
            preferred_element_type=jnp.float32,
        )
        gathered = jnp.einsum("sr,sqd->rqd", belongs_f, blended, precision=lax.Precision.HIGHEST)
        rescale = jnp.exp(peaks - raised)
        return (
            (raised, totals * rescale + row_sums, weighted * rescale[..., None] + gathered),
            None,
        )

    start_state = (
        jnp.full((requests, qcount), masked, jnp.float32),
        jnp.zeros((requests, qcount), jnp.float32),
        jnp.zeros((requests, qcount, head_dim), jnp.float32),
    )
    pieces = (
        key_rows_all,
        value_rows_all,
        block_owner_list.reshape(nsteps, stride),
        filled.reshape(nsteps, stride),
        usable.reshape(nsteps, stride, token_count),
    )
    return lax.scan(advance, start_state, pieces)[0]


def draft_partial(grouped, draft_keys, draft_values, current_replica, head_base):
    requests, qcount, head_dim = grouped.shape
    per_token = qcount // DRAFT
    rows_loc = draft_keys.shape[0]
    kv_head = head_base // 2
    own_keys = lax.dynamic_slice_in_dim(draft_keys, kv_head * head_dim, head_dim, 2)
    own_vals = lax.dynamic_slice_in_dim(draft_values, kv_head * head_dim, head_dim, 2)
    own_q = lax.dynamic_slice_in_dim(grouped, current_replica * rows_loc, rows_loc, 0).reshape(
        rows_loc, DRAFT, per_token, head_dim
    )
    inv_root = 1.0 / math.sqrt(head_dim)
    scores = (
        jnp.einsum("rigd,rjd->rigj", own_q, own_keys, preferred_element_type=jnp.float32) * inv_root
    )
    causal = jnp.arange(DRAFT)[None, :] <= jnp.arange(DRAFT)[:, None]
    causal_flat = jnp.broadcast_to(causal[:, None, :], (DRAFT, per_token, DRAFT)).reshape(
        qcount, DRAFT
    )
    scores = jnp.where(causal_flat, scores.reshape(rows_loc, qcount, DRAFT), masked)
    peaks = jnp.max(scores, axis=-1)
    weights = jnp.where(causal_flat, jnp.exp(scores - peaks[..., None]), 0.0)
    totals = jnp.sum(weights, axis=-1)
    weighted = jnp.einsum(
        "rqj,rjd->rqd", weights.astype(jnp.bfloat16), own_vals, preferred_element_type=jnp.float32
    )
    include = head_base % 2 == 0
    peaks = jnp.where(include, peaks, masked)
    totals = jnp.where(include, totals, 0.0)
    weighted = jnp.where(include, weighted, 0.0)
    first_row = current_replica * rows_loc
    full_peaks = lax.dynamic_update_slice_in_dim(
        jnp.full((requests, qcount), masked, jnp.float32), peaks, first_row, 0
    )
    full_totals = lax.dynamic_update_slice_in_dim(
        jnp.zeros((requests, qcount), jnp.float32), totals, first_row, 0
    )
    full_weighted = lax.dynamic_update_slice_in_dim(
        jnp.zeros((requests, qcount, head_dim), jnp.float32), weighted, first_row, 0
    )
    return (full_peaks, full_totals, full_weighted)


def general_shards(old_keys, old_values, old_block, new_slot, lengths, queries, draft_keys, draft_values):
    replica_count = lax.axis_size("inst")
    current_replica = lax.axis_index("inst")
    me_head = lax.axis_index("head")
    entries = old_keys.shape[1]
    head_dim = old_keys.shape[3]
    head_base = me_head * entries
    block_capacity = new_slot.shape[0]
    slots_per_replica = block_capacity // replica_count
    destination_replica = jnp.where(
        old_block >= 0, new_slot[jnp.clip(old_block, 0, block_capacity - 1)], block_capacity
    )
    trailing_tokens = old_keys.shape[1:]
    outgoing_keys = (
        jnp.zeros((block_capacity,) + trailing_tokens, old_keys.dtype)
        .at[destination_replica]
        .set(old_keys, mode="drop")
    )
    outgoing_values = (
        jnp.zeros((block_capacity,) + trailing_tokens, old_values.dtype)
        .at[destination_replica]
        .set(old_values, mode="drop")
    )
    outgoing_keys = outgoing_keys.reshape((replica_count, slots_per_replica) + trailing_tokens)
    outgoing_values = outgoing_values.reshape((replica_count, slots_per_replica) + trailing_tokens)
    inbox_k, inbox_v = (
        lax.all_to_all(outgoing_keys, "inst", split_axis=0, concat_axis=0, tiled=True),
        lax.all_to_all(outgoing_values, "inst", split_axis=0, concat_axis=0, tiled=True),
    )
    moved_keys = jnp.sum(inbox_k, axis=0)
    moved_values = jnp.sum(inbox_v, axis=0)
    local_heads = queries.shape[2] // head_dim
    requests = queries.shape[0]
    locally_present = (
        jnp.zeros((block_capacity,), jnp.int32)
        .at[new_slot]
        .set(jnp.arange(block_capacity, dtype=jnp.int32))
    )
    block_list = lax.dynamic_slice_in_dim(
        locally_present, current_replica * slots_per_replica, slots_per_replica
    )
    split_tokens = False
    if local_heads < GROUP:
        is_lower = me_head % 2 == 0
        partner = partner_2(queries, "head", 0)
        grouped = jnp.where(
            is_lower,
            jnp.concatenate([queries, partner], axis=2),
            jnp.concatenate([partner, queries], axis=2),
        )
        split_tokens = True
    else:
        grouped = queries
    qcount = grouped.shape[2] // head_dim
    grouped = grouped.reshape(requests, DRAFT * qcount, head_dim)
    cached = cache_partial(moved_keys, moved_values, block_list, lengths, grouped, head_base)
    drafted = draft_partial(grouped, draft_keys, draft_values, current_replica, head_base)
    peaks, totals, weighted = join_partials(cached, drafted)
    if split_tokens:
        peaks = peaks.reshape(requests, DRAFT, 2, local_heads)
        totals = totals.reshape(requests, DRAFT, 2, local_heads)
        weighted = weighted.reshape(requests, DRAFT, 2, local_heads, head_dim)
        is_first = me_head % 2 == 0
        own_peaks = jnp.where(is_first, peaks[:, :, 0], peaks[:, :, 1])
        own_totals = jnp.where(is_first, totals[:, :, 0], totals[:, :, 1])
        own_weighted = jnp.where(is_first, weighted[:, :, 0], weighted[:, :, 1])
        other_peaks = jnp.where(is_first, peaks[:, :, 1], peaks[:, :, 0])
        other_totals = jnp.where(is_first, totals[:, :, 1], totals[:, :, 0])
        other_weighted = jnp.where(is_first, weighted[:, :, 1], weighted[:, :, 0])
        received = partner_2((other_peaks, other_totals, other_weighted), "head", 0)
        peaks, totals, weighted = join_partials((own_peaks, own_totals, own_weighted), received)
    else:
        peaks = peaks.reshape(requests, DRAFT, local_heads)
        totals = totals.reshape(requests, DRAFT, local_heads)
        weighted = weighted.reshape(requests, DRAFT, local_heads, head_dim)
    top_score = lax.pmax(peaks, "inst")
    factor = jnp.exp(peaks - top_score)
    totals, weighted = lax.psum((totals * factor, weighted * factor[..., None]), "inst")
    attended = (
        (weighted / totals[..., None])
        .astype(jnp.bfloat16)
        .reshape(requests, DRAFT, local_heads * head_dim)
    )
    return (moved_keys, moved_values, attended)


UNROLL = 4
SEND_SPLIT = 2


def flag_kernel(n, flag_ref, out_ref, send_sem, recv_sem):
    me = lax.axis_index("inst")
    barrier = pltpu.get_barrier_semaphore()
    for step in range(1, n):
        pl.semaphore_signal(
            barrier,
            inc=1,
            device_id={"inst": lax.rem(me + step, n)},
            device_id_type=pl.DeviceIdType.MESH,
        )
    pl.semaphore_wait(barrier, n - 1)
    copies = []
    for step in range(1, n):
        copy = pltpu.make_async_remote_copy(
            src_ref=flag_ref,
            dst_ref=out_ref.at[step],
            send_sem=send_sem.at[step],
            recv_sem=recv_sem.at[step],
            device_id={"inst": lax.rem(me + step, n)},
            device_id_type=pl.DeviceIdType.MESH,
        )
        copy.start()
        copies.append(copy)
    out_ref[0] = flag_ref[...]
    for copy in copies:
        copy.wait()


def find_holder(old_block, n):
    me = lax.axis_index("inst")
    mine = jnp.broadcast_to((jnp.max(old_block) >= 0).astype(jnp.int32), (8, 128))
    flags = pl.pallas_call(
        functools.partial(flag_kernel, n),
        out_shape=jax.ShapeDtypeStruct((n, 8, 128), jnp.int32),
        in_specs=[pl.BlockSpec(memory_space=pltpu.VMEM)],
        out_specs=pl.BlockSpec(memory_space=pltpu.VMEM),
        scratch_shapes=[pltpu.SemaphoreType.DMA((n,)), pltpu.SemaphoreType.DMA((n,))],
        compiler_params=pltpu.CompilerParams(collective_id=0, has_side_effects=True),
    )(mine)
    origin = (me - jnp.arange(n, dtype=jnp.int32) + n) % n
    return jnp.sum(origin * flags[:, 0, 0])


def tables(old_block, new_slot, lengths):
    blocks = new_slot.shape[0]
    requests = lengths.shape[0]
    ids = jnp.arange(blocks, dtype=jnp.int32)
    spots = jnp.arange(old_block.shape[0], dtype=jnp.int32)
    source = jnp.sum(jnp.where(old_block[None, :] == ids[:, None], spots[None, :], 0), axis=1)
    placed = jnp.sum(jnp.where(old_block[:, None] == ids[None, :], new_slot[None, :] + 1, 0), axis=1) - 1
    by_slot = jnp.sum(jnp.where(placed[None, :] == ids[:, None], spots[None, :], 0), axis=1)
    counts = (lengths + BLK - 1) // BLK
    reqs = jnp.arange(requests, dtype=jnp.int32)
    ends = jnp.sum(jnp.where(reqs[None, :] <= reqs[:, None], counts[None, :], 0), axis=1)
    starts = ends - counts
    inside = (starts[None, :] <= ids[:, None]) & (ids[:, None] < ends[None, :])
    owner = jnp.sum(jnp.where(inside, reqs[None, :], 0), axis=1)
    left = lengths[None, :] - (ids[:, None] - starts[None, :]) * BLK
    live = jnp.minimum(jnp.sum(jnp.where(inside, left, 0), axis=1), BLK)
    first = jnp.sum(jnp.where(inside & (starts[None, :] == ids[:, None]), 1, 0), axis=1)
    last = jnp.pad(ends - 1, (0, blocks - requests))
    return jnp.stack([source, by_slot, owner, live, first, last])


def fused_kernel(
    holder,
    tab,
    keys_hbm,
    values_hbm,
    queries_hbm,
    dkeys_hbm,
    dvals_hbm,
    mk_out,
    mv_out,
    att_out,
    kbuf,
    vbuf,
    qbuf,
    dk,
    dv,
    send_k,
    send_v,
    relay,
    per_block,
    att,
    m_ref,
    l_ref,
    acc_ref,
    load_sem,
    keep_sem,
    draft_send,
    draft_recv,
    blk_send,
    blk_recv,
    fwd_send,
    fwd_recv,
    att_send,
    att_recv,
    pass_send,
    pass_recv,
):
    me = lax.axis_index("inst")
    head = lax.axis_index("head")
    mesh_id = pl.DeviceIdType.MESH
    cross_x, cross_y, far = holder ^ 1, holder ^ 2, holder ^ 3
    insts = 4
    blocks = kbuf.shape[0]
    per_inst = blocks // insts
    head_dim = kbuf.shape[3]
    requests = qbuf.shape[0]
    rows_loc = requests // insts
    local_heads = qbuf.shape[2] // head_dim
    units = 4
    unit = per_inst // units
    nchunk = 8
    chunk = requests // nchunk
    half_chunks = nchunk // 2

    barrier = pltpu.get_barrier_semaphore()
    for step in range(1, insts):
        pl.semaphore_signal(
            barrier, inc=1, device_id={"inst": lax.rem(me + step, insts)}, device_id_type=mesh_id
        )
    pl.semaphore_wait(barrier, insts - 1)

    lanes = pl.ds(pl.multiple_of(head * head_dim, head_dim), head_dim)

    def draft_copies(origin):
        rows = pl.ds(origin * rows_loc, rows_loc)
        return [
            pltpu.make_async_remote_copy(
                src_ref=src.at[:, :, lanes],
                dst_ref=dst.at[rows],
                send_sem=draft_send.at[n],
                recv_sem=draft_recv.at[origin, n],
                device_id={"inst": holder},
                device_id_type=mesh_id,
            )
            for n, (src, dst) in enumerate(((dkeys_hbm, dk), (dvals_hbm, dv)))
        ]

    def out_of(n):
        return (mk_out, mv_out)[n // units].at[pl.ds((n % units) * unit, unit)]

    def staged(inst, n):
        return (send_k, send_v)[n // units].at[pl.ds(inst * per_inst + (n % units) * unit, unit)]

    def block_copy(inst, n):
        if inst == far:
            to = cross_x if n % 2 == 0 else cross_y
            dst = relay.at[n // 2]
        else:
            to = inst
            dst = out_of(n)
        return pltpu.make_async_remote_copy(
            src_ref=staged(inst, n),
            dst_ref=dst,
            send_sem=blk_send.at[inst, n],
            recv_sem=blk_recv.at[inst, n],
            device_id={"inst": to},
            device_id_type=mesh_id,
        )

    def relay_copy(n):
        return pltpu.make_async_remote_copy(
            src_ref=relay.at[n // 2],
            dst_ref=out_of(n),
            send_sem=fwd_send.at[n],
            recv_sem=fwd_recv.at[n],
            device_id={"inst": far},
            device_id_type=mesh_id,
        )

    def att_copy(src, c, to, send, recv):
        rows = pl.ds(c * chunk, chunk)
        return pltpu.make_async_remote_copy(
            src_ref=src.at[rows],
            dst_ref=att_out.at[rows],
            send_sem=send.at[c],
            recv_sem=recv.at[c],
            device_id={"inst": to},
            device_id_type=mesh_id,
        )

    def first_hop(c):
        return att_copy(att, c, cross_x if c < half_chunks else cross_y, att_send, att_recv)

    def second_hop(c):
        return att_copy(att_out, c, far, pass_send, pass_recv)

    def third_hop(c):
        return att_copy(
            att_out, c, cross_y if c < half_chunks else cross_x, att_send, att_recv
        )

    @pl.when(me == holder)
    def _():
        loads = [
            pltpu.make_async_copy(src, dst, load_sem.at[n])
            for n, (src, dst) in enumerate(
                (
                    (keys_hbm, kbuf),
                    (values_hbm, vbuf),
                    (queries_hbm, qbuf),
                    (dkeys_hbm.at[:, :, lanes], dk.at[pl.ds(holder * rows_loc, rows_loc)]),
                    (dvals_hbm.at[:, :, lanes], dv.at[pl.ds(holder * rows_loc, rows_loc)]),
                )
            )
        ]
        for load in loads:
            load.start()

        def fill(src, dst, inst):
            def one(i, _):
                slot = inst * per_inst + i
                dst[slot] = src[tab[1, slot]]
                return 0

            lax.fori_loop(0, per_inst, one, 0)

        loads[0].wait()
        fill(kbuf, send_k, far)
        fill(kbuf, send_k, cross_x)
        for n in range(units):
            block_copy(far, n).start()
        loads[1].wait()
        fill(vbuf, send_v, far)
        fill(kbuf, send_k, cross_y)
        for n in range(units, 2 * units):
            block_copy(far, n).start()
        fill(vbuf, send_v, cross_x)
        fill(vbuf, send_v, cross_y)
        for n in range(SEND_SPLIT):
            block_copy(cross_x, n).start()
            block_copy(cross_y, n).start()
        fill(kbuf, send_k, holder)
        fill(vbuf, send_v, holder)

        for load in loads[2:]:
            load.wait()
        for origin in (cross_x, cross_y, far):
            for copy in draft_copies(origin):
                copy.wait_recv()

        inv_root = 1.0 / math.sqrt(head_dim)
        rows = DRAFT * local_heads
        cols = BLK + DRAFT
        col = lax.broadcasted_iota(jnp.int32, (rows, cols), 1)
        row = lax.broadcasted_iota(jnp.int32, (rows, cols), 0)
        causal = (col >= BLK) & (col - BLK <= row % DRAFT)
        causal_i = causal.astype(jnp.int32)
        m_ref[...] = jnp.full(m_ref.shape, masked, jnp.float32)
        l_ref[...] = jnp.zeros(l_ref.shape, jnp.float32)
        acc_ref[...] = jnp.zeros(acc_ref.shape, jnp.float32)

        def attend(step, _):
            parts = []
            for u in range(UNROLL):
                g = step * UNROLL + u
                spot, owner, live, first = tab[0, g], tab[2, g], tab[3, g], tab[4, g]
                q = qbuf[owner]
                q = jnp.concatenate(
                    [q[:, j * head_dim : (j + 1) * head_dim] for j in range(local_heads)], axis=0
                )
                k = jnp.concatenate([kbuf[spot].reshape(BLK, head_dim), dk[owner]], axis=0)
                v = jnp.concatenate([vbuf[spot].reshape(BLK, head_dim), dv[owner]], axis=0)
                s = (
                    lax.dot_general(
                        q, k, (((1,), (1,)), ((), ())), preferred_element_type=jnp.float32
                    )
                    * inv_root
                )
                usable = (col < live) | (causal_i * first > 0)
                s = jnp.where(usable, s, masked)
                m = jnp.max(s, axis=1, keepdims=True)
                p = jnp.exp(s - m)
                l = jnp.sum(p, axis=1, keepdims=True)
                acc = jnp.dot(p.astype(jnp.bfloat16), v, preferred_element_type=jnp.float32)
                parts.append((g, first, m, l, acc))
            m_run, l_run, acc_run = m_ref[...], l_ref[...], acc_ref[...]
            for g, first, m, l, acc in parts:
                m_run = jnp.where(first > 0, masked, m_run)
                raised = jnp.maximum(m_run, m)
                old = jnp.exp(m_run - raised)
                new = jnp.exp(m - raised)
                m_run = raised
                l_run = l_run * old + l * new
                acc_run = acc_run * old + acc * new
                out = (acc_run / l_run).astype(jnp.bfloat16)
                for j in range(local_heads):
                    per_block[g, :, j * head_dim : (j + 1) * head_dim] = out[
                        j * DRAFT : (j + 1) * DRAFT
                    ]
            m_ref[...], l_ref[...], acc_ref[...] = m_run, l_run, acc_run
            return 0

        lax.fori_loop(0, blocks // UNROLL, attend, 0)

        def pick(r, _):
            att[r] = per_block[tab[5, r]]
            return 0

        lax.fori_loop(0, requests, pick, 0)
        keeps = [
            pltpu.make_async_copy(staged(holder, n), out_of(n), keep_sem.at[n])
            for n in range(2 * units)
        ]
        for keep in keeps:
            keep.start()
        for c in range(half_chunks):
            first_hop(c).start()
            first_hop(c + half_chunks).start()
        for n in range(SEND_SPLIT, 2 * units):
            block_copy(cross_x, n).start()
            block_copy(cross_y, n).start()
        own = pltpu.make_async_copy(att, att_out, load_sem.at[5])
        own.start()
        for keep in keeps:
            keep.wait()
        own.wait()
        for n in range(2 * units):
            for inst in (far, cross_x, cross_y):
                block_copy(inst, n).wait_send()
        for c in range(nchunk):
            first_hop(c).wait_send()

    @pl.when(me != holder)
    def _():
        for copy in draft_copies(me):
            copy.start()

    for side, relayed, mine, theirs in (
        (cross_x, range(0, 2 * units, 2), range(half_chunks), range(half_chunks, nchunk)),
        (cross_y, range(1, 2 * units, 2), range(half_chunks, nchunk), range(half_chunks)),
    ):

        @pl.when(me == side)
        def _(side=side, relayed=relayed, mine=mine, theirs=theirs):
            for n in relayed:
                block_copy(far, n).wait_recv()
                relay_copy(n).start()
            for c in mine:
                first_hop(c).wait_recv()
                second_hop(c).start()
            for n in range(2 * units):
                block_copy(side, n).wait_recv()
            for c in theirs:
                third_hop(c).wait_recv()
            for n in relayed:
                relay_copy(n).wait_send()
            for c in mine:
                second_hop(c).wait_send()

    @pl.when(me == far)
    def _():
        for n in range(2 * units):
            relay_copy(n).wait_recv()
        for c in range(half_chunks):
            for half in (c, c + half_chunks):
                second_hop(half).wait_recv()
                third_hop(half).start()
        for c in range(nchunk):
            third_hop(c).wait_send()

    @pl.when(me != holder)
    def _():
        for copy in draft_copies(me):
            copy.wait_send()


def fused(holder, tab, old_keys, old_values, queries, draft_keys, draft_values):
    blocks = old_keys.shape[0]
    per_inst = blocks // 4
    requests, draft, width = queries.shape
    head_dim = old_keys.shape[3]
    rows = draft * (width // head_dim)
    block = old_keys.shape[1:]
    units = 4
    dma = pltpu.SemaphoreType.DMA
    any_space = pl.BlockSpec(memory_space=pl.ANY)
    bf = jnp.bfloat16
    return pl.pallas_call(
        functools.partial(fused_kernel, holder),
        out_shape=(
            jax.ShapeDtypeStruct((per_inst,) + block, bf),
            jax.ShapeDtypeStruct((per_inst,) + block, bf),
            jax.ShapeDtypeStruct(queries.shape, bf),
        ),
        in_specs=[pl.BlockSpec(memory_space=pltpu.SMEM)] + [any_space] * 5,
        out_specs=(any_space,) * 3,
        scratch_shapes=[
            pltpu.VMEM((blocks,) + block, bf),
            pltpu.VMEM((blocks,) + block, bf),
            pltpu.VMEM(queries.shape, bf),
            pltpu.VMEM((requests, draft, head_dim), bf),
            pltpu.VMEM((requests, draft, head_dim), bf),
            pltpu.VMEM((blocks,) + block, bf),
            pltpu.VMEM((blocks,) + block, bf),
            pltpu.VMEM((units, per_inst // units) + block, bf),
            pltpu.VMEM((blocks, draft, width), bf),
            pltpu.VMEM(queries.shape, bf),
            pltpu.VMEM((rows, head_dim), jnp.float32),
            pltpu.VMEM((rows, head_dim), jnp.float32),
            pltpu.VMEM((rows, head_dim), jnp.float32),
            dma((6,)),
            dma((2 * units,)),
            dma((2,)),
            dma((4, 2)),
            dma((4, 2 * units)),
            dma((4, 2 * units)),
            dma((2 * units,)),
            dma((2 * units,)),
            dma((8,)),
            dma((8,)),
            dma((8,)),
            dma((8,)),
        ],
        compiler_params=pltpu.CompilerParams(
            collective_id=1 + holder, has_side_effects=True, vmem_limit_bytes=60 * 1024 * 1024
        ),
    )(tab, old_keys, old_values, queries, draft_keys, draft_values)


def shards(old_keys, old_values, old_block, new_slot, lengths, queries, draft_keys, draft_values):
    insts = lax.axis_size("inst")
    plain = (
        insts == 4
        and old_block.shape[0] == new_slot.shape[0]
        and old_keys.shape[1] * old_keys.shape[2] == BLK
        and queries.shape[2] // old_keys.shape[3] == GROUP
        and lengths.shape[0] % 8 == 0
        and new_slot.shape[0] % 16 == 0
        and lengths.shape[0] <= new_slot.shape[0]
    )
    if not plain:
        return general_shards(
            old_keys, old_values, old_block, new_slot, lengths, queries, draft_keys, draft_values
        )
    holder = find_holder(old_block, insts)
    tab = tables(old_block, new_slot, lengths)
    return lax.switch(
        holder,
        [functools.partial(fused, h) for h in range(insts)],
        tab,
        old_keys,
        old_values,
        queries,
        draft_keys,
        draft_values,
    )


def solution(mesh):
    placed = (
        P("inst", "head", None, None),
        P("inst", "head", None, None),
        P("inst"),
        P(),
        P(),
        P(None, None, "head"),
        P("inst", None, None),
        P("inst", None, None),
    )
    return jax.shard_map(
        shards,
        mesh=mesh,
        in_specs=placed,
        out_specs=(
            P("inst", "head", None, None),
            P("inst", "head", None, None),
            P(None, None, "head"),
        ),
        check_vma=False,
    )
```

```python
import functools
import math

import jax
import jax.numpy as jnp
from jax import lax
from jax.experimental import pallas as pl
from jax.experimental.pallas import tpu as pltpu
from jax.sharding import PartitionSpec as P

GROUP = 8
BLK = 128
DRAFT = 16


masked = -1e30


def partner_2(block, axis, stride):
    count = lax.axis_size(axis)
    route = []
    for low in range(count):
        high = low | 1 << stride
        if high != low and high < count:
            route += [(low, high), (high, low)]
    return lax.ppermute(block, axis, route)


def join_partials(earlier, later):
    raised = jnp.maximum(earlier[0], later[0])
    keep_early = jnp.exp(earlier[0] - raised)
    keep_late = jnp.exp(later[0] - raised)
    totals = earlier[1] * keep_early + later[1] * keep_late
    weighted = earlier[2] * keep_early[..., None] + later[2] * keep_late[..., None]
    return (raised, totals, weighted)


def cache_partial(key_cache, value_cache, block_list, lengths, grouped, head_base):
    slot_count, entries, half_len, head_dim = key_cache.shape
    requests, qcount, _ = grouped.shape
    inv_root = 1.0 / math.sqrt(head_dim)
    counts = (lengths + BLK - 1) // BLK
    starts = jnp.cumsum(counts) - counts
    filled = block_list >= 0
    block_owner_list = (
        jnp.sum((starts[None, :] <= block_list[:, None]).astype(jnp.int32), axis=1) - 1
    )
    block_owner_list = jnp.clip(block_owner_list, 0, requests - 1)
    offset = block_list - starts[block_owner_list]
    halves = (head_base + jnp.arange(entries, dtype=jnp.int32)) % 2
    within = (halves[:, None] * half_len + jnp.arange(half_len, dtype=jnp.int32)[None, :]).reshape(
        entries * half_len
    )
    positions = offset[:, None] * BLK + within[None, :]
    usable = filled[:, None] & (positions < lengths[block_owner_list][:, None])
    stride = math.gcd(slot_count, 64)
    nsteps = slot_count // stride
    token_count = entries * half_len
    key_rows_all = key_cache.reshape(nsteps, stride, token_count, head_dim)
    value_rows_all = value_cache.reshape(nsteps, stride, token_count, head_dim)
    request_ids = jnp.arange(requests, dtype=jnp.int32)

    def advance(state_now, pieces):
        peaks, totals, weighted = state_now
        key_rows, value_rows, rows_owner, rows_filled, rows_usable = pieces
        picked = grouped[rows_owner]
        scores = (
            jnp.einsum("sqd,std->sqt", picked, key_rows, preferred_element_type=jnp.float32)
            * inv_root
        )
        scores = jnp.where(rows_usable[:, None, :], scores, masked)
        belongs = (rows_owner[:, None] == request_ids[None, :]) & rows_filled[:, None]
        slot_peaks = jnp.max(scores, axis=-1)
        block_peak = jnp.max(jnp.where(belongs[:, :, None], slot_peaks[:, None, :], masked), axis=0)
        raised = jnp.maximum(peaks, block_peak)
        weights = jnp.where(
            rows_usable[:, None, :], jnp.exp(scores - raised[rows_owner][:, :, None]), 0.0
        )
        belongs_f = belongs.astype(jnp.float32)
        row_sums = jnp.dot(
            belongs_f.T,
            jnp.sum(weights, axis=-1),
            precision=lax.Precision.HIGHEST,
            preferred_element_type=jnp.float32,
        )
        blended = jnp.einsum(
            "sqt,std->sqd",
            weights.astype(jnp.bfloat16),
            value_rows,
            preferred_element_type=jnp.float32,
        )
        gathered = jnp.einsum("sr,sqd->rqd", belongs_f, blended, precision=lax.Precision.HIGHEST)
        rescale = jnp.exp(peaks - raised)
        return (
            (raised, totals * rescale + row_sums, weighted * rescale[..., None] + gathered),
            None,
        )

    start_state = (
        jnp.full((requests, qcount), masked, jnp.float32),
        jnp.zeros((requests, qcount), jnp.float32),
        jnp.zeros((requests, qcount, head_dim), jnp.float32),
    )
    pieces = (
        key_rows_all,
        value_rows_all,
        block_owner_list.reshape(nsteps, stride),
        filled.reshape(nsteps, stride),
        usable.reshape(nsteps, stride, token_count),
    )
    return lax.scan(advance, start_state, pieces)[0]


def draft_partial(grouped, draft_keys, draft_values, current_replica, head_base):
    requests, qcount, head_dim = grouped.shape
    per_token = qcount // DRAFT
    rows_loc = draft_keys.shape[0]
    kv_head = head_base // 2
    own_keys = lax.dynamic_slice_in_dim(draft_keys, kv_head * head_dim, head_dim, 2)
    own_vals = lax.dynamic_slice_in_dim(draft_values, kv_head * head_dim, head_dim, 2)
    own_q = lax.dynamic_slice_in_dim(grouped, current_replica * rows_loc, rows_loc, 0).reshape(
        rows_loc, DRAFT, per_token, head_dim
    )
    inv_root = 1.0 / math.sqrt(head_dim)
    scores = (
        jnp.einsum("rigd,rjd->rigj", own_q, own_keys, preferred_element_type=jnp.float32) * inv_root
    )
    causal = jnp.arange(DRAFT)[None, :] <= jnp.arange(DRAFT)[:, None]
    causal_flat = jnp.broadcast_to(causal[:, None, :], (DRAFT, per_token, DRAFT)).reshape(
        qcount, DRAFT
    )
    scores = jnp.where(causal_flat, scores.reshape(rows_loc, qcount, DRAFT), masked)
    peaks = jnp.max(scores, axis=-1)
    weights = jnp.where(causal_flat, jnp.exp(scores - peaks[..., None]), 0.0)
    totals = jnp.sum(weights, axis=-1)
    weighted = jnp.einsum(
        "rqj,rjd->rqd", weights.astype(jnp.bfloat16), own_vals, preferred_element_type=jnp.float32
    )
    include = head_base % 2 == 0
    peaks = jnp.where(include, peaks, masked)
    totals = jnp.where(include, totals, 0.0)
    weighted = jnp.where(include, weighted, 0.0)
    first_row = current_replica * rows_loc
    full_peaks = lax.dynamic_update_slice_in_dim(
        jnp.full((requests, qcount), masked, jnp.float32), peaks, first_row, 0
    )
    full_totals = lax.dynamic_update_slice_in_dim(
        jnp.zeros((requests, qcount), jnp.float32), totals, first_row, 0
    )
    full_weighted = lax.dynamic_update_slice_in_dim(
        jnp.zeros((requests, qcount, head_dim), jnp.float32), weighted, first_row, 0
    )
    return (full_peaks, full_totals, full_weighted)


def general_shards(old_keys, old_values, old_block, new_slot, lengths, queries, draft_keys, draft_values):
    replica_count = lax.axis_size("inst")
    current_replica = lax.axis_index("inst")
    me_head = lax.axis_index("head")
    entries = old_keys.shape[1]
    head_dim = old_keys.shape[3]
    head_base = me_head * entries
    block_capacity = new_slot.shape[0]
    slots_per_replica = block_capacity // replica_count
    destination_replica = jnp.where(
        old_block >= 0, new_slot[jnp.clip(old_block, 0, block_capacity - 1)], block_capacity
    )
    trailing_tokens = old_keys.shape[1:]
    outgoing_keys = (
        jnp.zeros((block_capacity,) + trailing_tokens, old_keys.dtype)
        .at[destination_replica]
        .set(old_keys, mode="drop")
    )
    outgoing_values = (
        jnp.zeros((block_capacity,) + trailing_tokens, old_values.dtype)
        .at[destination_replica]
        .set(old_values, mode="drop")
    )
    outgoing_keys = outgoing_keys.reshape((replica_count, slots_per_replica) + trailing_tokens)
    outgoing_values = outgoing_values.reshape((replica_count, slots_per_replica) + trailing_tokens)
    inbox_k, inbox_v = (
        lax.all_to_all(outgoing_keys, "inst", split_axis=0, concat_axis=0, tiled=True),
        lax.all_to_all(outgoing_values, "inst", split_axis=0, concat_axis=0, tiled=True),
    )
    moved_keys = jnp.sum(inbox_k, axis=0)
    moved_values = jnp.sum(inbox_v, axis=0)
    local_heads = queries.shape[2] // head_dim
    requests = queries.shape[0]
    locally_present = (
        jnp.zeros((block_capacity,), jnp.int32)
        .at[new_slot]
        .set(jnp.arange(block_capacity, dtype=jnp.int32))
    )
    block_list = lax.dynamic_slice_in_dim(
        locally_present, current_replica * slots_per_replica, slots_per_replica
    )
    split_tokens = False
    if local_heads < GROUP:
        is_lower = me_head % 2 == 0
        partner = partner_2(queries, "head", 0)
        grouped = jnp.where(
            is_lower,
            jnp.concatenate([queries, partner], axis=2),
            jnp.concatenate([partner, queries], axis=2),
        )
        split_tokens = True
    else:
        grouped = queries
    qcount = grouped.shape[2] // head_dim
    grouped = grouped.reshape(requests, DRAFT * qcount, head_dim)
    cached = cache_partial(moved_keys, moved_values, block_list, lengths, grouped, head_base)
    drafted = draft_partial(grouped, draft_keys, draft_values, current_replica, head_base)
    peaks, totals, weighted = join_partials(cached, drafted)
    if split_tokens:
        peaks = peaks.reshape(requests, DRAFT, 2, local_heads)
        totals = totals.reshape(requests, DRAFT, 2, local_heads)
        weighted = weighted.reshape(requests, DRAFT, 2, local_heads, head_dim)
        is_first = me_head % 2 == 0
        own_peaks = jnp.where(is_first, peaks[:, :, 0], peaks[:, :, 1])
        own_totals = jnp.where(is_first, totals[:, :, 0], totals[:, :, 1])
        own_weighted = jnp.where(is_first, weighted[:, :, 0], weighted[:, :, 1])
        other_peaks = jnp.where(is_first, peaks[:, :, 1], peaks[:, :, 0])
        other_totals = jnp.where(is_first, totals[:, :, 1], totals[:, :, 0])
        other_weighted = jnp.where(is_first, weighted[:, :, 1], weighted[:, :, 0])
        received = partner_2((other_peaks, other_totals, other_weighted), "head", 0)
        peaks, totals, weighted = join_partials((own_peaks, own_totals, own_weighted), received)
    else:
        peaks = peaks.reshape(requests, DRAFT, local_heads)
        totals = totals.reshape(requests, DRAFT, local_heads)
        weighted = weighted.reshape(requests, DRAFT, local_heads, head_dim)
    top_score = lax.pmax(peaks, "inst")
    factor = jnp.exp(peaks - top_score)
    totals, weighted = lax.psum((totals * factor, weighted * factor[..., None]), "inst")
    attended = (
        (weighted / totals[..., None])
        .astype(jnp.bfloat16)
        .reshape(requests, DRAFT, local_heads * head_dim)
    )
    return (moved_keys, moved_values, attended)


UNROLL = 4
SEND_SPLIT = 2


def prep_kernel(n, old_ref, slot_ref, len_ref, tab_ref, flag, got, send_sem, recv_sem):
    me = lax.axis_index("inst")
    barrier = pltpu.get_barrier_semaphore()
    for step in range(1, n):
        pl.semaphore_signal(
            barrier,
            inc=1,
            device_id={"inst": lax.rem(me + step, n)},
            device_id_type=pl.DeviceIdType.MESH,
        )
    size = old_ref.shape[1]
    wide = (size, size)
    old = jnp.broadcast_to(old_ref[...], wide)
    filled = jnp.max(old[:8].astype(jnp.float32), axis=1, keepdims=True) >= 0.0
    flag[...] = jnp.broadcast_to(jnp.where(filled, me, 0), flag.shape)
    pl.semaphore_wait(barrier, n - 1)
    copies = []
    for step in range(1, n):
        copy = pltpu.make_async_remote_copy(
            src_ref=flag,
            dst_ref=got.at[step],
            send_sem=send_sem.at[step],
            recv_sem=recv_sem.at[step],
            device_id={"inst": lax.rem(me + step, n)},
            device_id_type=pl.DeviceIdType.MESH,
        )
        copy.start()
        copies.append(copy)

    r = lax.broadcasted_iota(jnp.int32, wide, 0)
    c = lax.broadcasted_iota(jnp.int32, wide, 1)

    def total(where, what, axis):
        return jnp.sum(jnp.where(where, what.astype(jnp.float32), 0.0), axis=axis, keepdims=True)

    old_t = old.T
    source = total(old_t == c, r, 0)
    placed = total(old_t == c, jnp.broadcast_to(slot_ref[...], wide), 1).astype(jnp.int32)
    placed = jnp.where(old_t >= 0, placed, -1)
    by_slot = total(placed == c, r, 0)
    length = jnp.broadcast_to(len_ref[...], wide)
    length_t = length.T
    counts = (length + (BLK - 1)) // BLK
    counts_t = (length_t + (BLK - 1)) // BLK
    ends = total(r <= c, counts_t, 0)
    ends_t = total(c <= r, counts, 1).astype(jnp.int32)
    starts_t = ends_t - counts_t
    inside = (starts_t <= c) & (c < ends_t)
    owner = total(inside, r, 0)
    live = jnp.minimum(total(inside, length_t - (c - starts_t) * BLK, 0), float(BLK))
    first = total(inside & (starts_t == c), jnp.ones(wide, jnp.int32), 0)
    rows = [source, by_slot, owner, live, first, ends - 1.0]
    for n_row, row in enumerate(rows):
        tab_ref[n_row : n_row + 1, :] = row.astype(jnp.int32)
    for copy in copies:
        copy.wait()
    holder = flag[0:1, :]
    for step in range(1, n):
        holder = holder + got[step, 0:1, :]
    tab_ref[6:7, :] = holder
    tab_ref[7:8, :] = holder


def prepare(old_block, new_slot, lengths, n):
    size = new_slot.shape[0]
    lengths = jnp.pad(lengths, (0, size - lengths.shape[0]))
    vmem = pl.BlockSpec(memory_space=pltpu.VMEM)
    return pl.pallas_call(
        functools.partial(prep_kernel, n),
        out_shape=jax.ShapeDtypeStruct((8, size), jnp.int32),
        in_specs=[vmem] * 3,
        out_specs=vmem,
        scratch_shapes=[
            pltpu.VMEM((8, size), jnp.int32),
            pltpu.VMEM((n, 8, size), jnp.int32),
            pltpu.SemaphoreType.DMA((n,)),
            pltpu.SemaphoreType.DMA((n,)),
        ],
        compiler_params=pltpu.CompilerParams(collective_id=0, has_side_effects=True),
    )(old_block.reshape(1, size), new_slot.reshape(1, size), lengths.reshape(1, size))


def fused_kernel(
    holder,
    tab,
    keys_hbm,
    values_hbm,
    queries_hbm,
    dkeys_hbm,
    dvals_hbm,
    mk_out,
    mv_out,
    att_out,
    kbuf,
    vbuf,
    qbuf,
    dk,
    dv,
    send_k,
    send_v,
    relay,
    per_block,
    att,
    m_ref,
    l_ref,
    acc_ref,
    load_sem,
    keep_sem,
    draft_send,
    draft_recv,
    blk_send,
    blk_recv,
    fwd_send,
    fwd_recv,
    att_send,
    att_recv,
    pass_send,
    pass_recv,
):
    me = lax.axis_index("inst")
    head = lax.axis_index("head")
    mesh_id = pl.DeviceIdType.MESH
    cross_x, cross_y, far = holder ^ 1, holder ^ 2, holder ^ 3
    insts = 4
    blocks = kbuf.shape[0]
    per_inst = blocks // insts
    head_dim = kbuf.shape[3]
    requests = qbuf.shape[0]
    rows_loc = requests // insts
    local_heads = qbuf.shape[2] // head_dim
    units = 4
    unit = per_inst // units
    nchunk = 8
    chunk = requests // nchunk
    half_chunks = nchunk // 2

    barrier = pltpu.get_barrier_semaphore()
    for step in range(1, insts):
        pl.semaphore_signal(
            barrier, inc=1, device_id={"inst": lax.rem(me + step, insts)}, device_id_type=mesh_id
        )

    lanes = pl.ds(pl.multiple_of(head * head_dim, head_dim), head_dim)

    loads = [
        pltpu.make_async_copy(src, dst, load_sem.at[n])
        for n, (src, dst) in enumerate(
            (
                (keys_hbm, kbuf),
                (values_hbm, vbuf),
                (queries_hbm, qbuf),
                (dkeys_hbm.at[:, :, lanes], dk.at[pl.ds(holder * rows_loc, rows_loc)]),
                (dvals_hbm.at[:, :, lanes], dv.at[pl.ds(holder * rows_loc, rows_loc)]),
            )
        )
    ]

    @pl.when(me == holder)
    def _():
        loads[0].start()

    pl.semaphore_wait(barrier, insts - 1)

    def draft_copies(origin):
        rows = pl.ds(origin * rows_loc, rows_loc)
        return [
            pltpu.make_async_remote_copy(
                src_ref=src.at[:, :, lanes],
                dst_ref=dst.at[rows],
                send_sem=draft_send.at[n],
                recv_sem=draft_recv.at[origin, n],
                device_id={"inst": holder},
                device_id_type=mesh_id,
            )
            for n, (src, dst) in enumerate(((dkeys_hbm, dk), (dvals_hbm, dv)))
        ]

    def out_of(n):
        return (mk_out, mv_out)[n // units].at[pl.ds((n % units) * unit, unit)]

    def staged(inst, n):
        return (send_k, send_v)[n // units].at[pl.ds(inst * per_inst + (n % units) * unit, unit)]

    def block_copy(inst, n):
        if inst == far:
            to = cross_x if n % 2 == 0 else cross_y
            dst = relay.at[n // 2]
        else:
            to = inst
            dst = out_of(n)
        return pltpu.make_async_remote_copy(
            src_ref=staged(inst, n),
            dst_ref=dst,
            send_sem=blk_send.at[inst, n],
            recv_sem=blk_recv.at[inst, n],
            device_id={"inst": to},
            device_id_type=mesh_id,
        )

    def relay_copy(n):
        return pltpu.make_async_remote_copy(
            src_ref=relay.at[n // 2],
            dst_ref=out_of(n),
            send_sem=fwd_send.at[n],
            recv_sem=fwd_recv.at[n],
            device_id={"inst": far},
            device_id_type=mesh_id,
        )

    def att_copy(src, c, to, send, recv):
        rows = pl.ds(c * chunk, chunk)
        return pltpu.make_async_remote_copy(
            src_ref=src.at[rows],
            dst_ref=att_out.at[rows],
            send_sem=send.at[c],
            recv_sem=recv.at[c],
            device_id={"inst": to},
            device_id_type=mesh_id,
        )

    def first_hop(c):
        return att_copy(att, c, cross_x if c < half_chunks else cross_y, att_send, att_recv)

    def second_hop(c):
        return att_copy(att_out, c, far, pass_send, pass_recv)

    def third_hop(c):
        return att_copy(
            att_out, c, cross_y if c < half_chunks else cross_x, att_send, att_recv
        )

    @pl.when(me == holder)
    def _():
        def fill(src, dst, inst):
            def one(i, _):
                slot = inst * per_inst + i
                dst[slot] = src[tab[1, slot]]
                return 0

            lax.fori_loop(0, per_inst, one, 0)

        loads[0].wait()
        loads[1].start()
        fill(kbuf, send_k, far)
        fill(kbuf, send_k, cross_x)
        for n in range(units):
            block_copy(far, n).start()
        fill(kbuf, send_k, cross_y)
        for n in range(SEND_SPLIT):
            block_copy(cross_x, n).start()
            block_copy(cross_y, n).start()
        loads[1].wait()
        for load in loads[2:]:
            load.start()
        fill(vbuf, send_v, far)
        fill(vbuf, send_v, cross_x)
        for n in range(units, 2 * units):
            block_copy(far, n).start()
        fill(vbuf, send_v, cross_y)
        fill(kbuf, send_k, holder)
        fill(vbuf, send_v, holder)

        for load in loads[2:]:
            load.wait()
        for origin in (cross_x, cross_y, far):
            for copy in draft_copies(origin):
                copy.wait_recv()

        inv_root = 1.0 / math.sqrt(head_dim)
        rows = DRAFT * local_heads
        cols = BLK + DRAFT
        col = lax.broadcasted_iota(jnp.int32, (rows, cols), 1)
        row = lax.broadcasted_iota(jnp.int32, (rows, cols), 0)
        causal = (col >= BLK) & (col - BLK <= row % DRAFT)
        causal_i = causal.astype(jnp.int32)
        m_ref[...] = jnp.full(m_ref.shape, masked, jnp.float32)
        l_ref[...] = jnp.zeros(l_ref.shape, jnp.float32)
        acc_ref[...] = jnp.zeros(acc_ref.shape, jnp.float32)

        def attend(step, _):
            parts = []
            for u in range(UNROLL):
                g = step * UNROLL + u
                spot, owner, live, first = tab[0, g], tab[2, g], tab[3, g], tab[4, g]
                q = qbuf[owner]
                q = jnp.concatenate(
                    [q[:, j * head_dim : (j + 1) * head_dim] for j in range(local_heads)], axis=0
                )
                k = jnp.concatenate([kbuf[spot].reshape(BLK, head_dim), dk[owner]], axis=0)
                v = jnp.concatenate([vbuf[spot].reshape(BLK, head_dim), dv[owner]], axis=0)
                s = (
                    lax.dot_general(
                        q, k, (((1,), (1,)), ((), ())), preferred_element_type=jnp.float32
                    )
                    * inv_root
                )
                usable = (col < live) | (causal_i * first > 0)
                s = jnp.where(usable, s, masked)
                m = jnp.max(s, axis=1, keepdims=True)
                p = jnp.exp(s - m)
                l = jnp.sum(p, axis=1, keepdims=True)
                acc = jnp.dot(p.astype(jnp.bfloat16), v, preferred_element_type=jnp.float32)
                parts.append((g, first, m, l, acc))
            m_run, l_run, acc_run = m_ref[...], l_ref[...], acc_ref[...]
            for g, first, m, l, acc in parts:
                m_run = jnp.where(first > 0, masked, m_run)
                raised = jnp.maximum(m_run, m)
                old = jnp.exp(m_run - raised)
                new = jnp.exp(m - raised)
                m_run = raised
                l_run = l_run * old + l * new
                acc_run = acc_run * old + acc * new
                out = (acc_run / l_run).astype(jnp.bfloat16)
                for j in range(local_heads):
                    per_block[g, :, j * head_dim : (j + 1) * head_dim] = out[
                        j * DRAFT : (j + 1) * DRAFT
                    ]
            m_ref[...], l_ref[...], acc_ref[...] = m_run, l_run, acc_run
            return 0

        lax.fori_loop(0, blocks // UNROLL, attend, 0)

        def pick(r, _):
            att[r] = per_block[tab[5, r]]
            return 0

        lax.fori_loop(0, requests, pick, 0)
        keeps = [
            pltpu.make_async_copy(staged(holder, n), out_of(n), keep_sem.at[n])
            for n in range(2 * units)
        ]
        for keep in keeps:
            keep.start()
        for c in range(half_chunks):
            first_hop(c).start()
            first_hop(c + half_chunks).start()
        for n in range(SEND_SPLIT, 2 * units):
            block_copy(cross_x, n).start()
            block_copy(cross_y, n).start()
        own = pltpu.make_async_copy(att, att_out, load_sem.at[5])
        own.start()
        for keep in keeps:
            keep.wait()
        own.wait()
        for n in range(2 * units):
            for inst in (far, cross_x, cross_y):
                block_copy(inst, n).wait_send()
        for c in range(nchunk):
            first_hop(c).wait_send()

    @pl.when(me != holder)
    def _():
        for copy in draft_copies(me):
            copy.start()

    for side, relayed, mine, theirs in (
        (cross_x, range(0, 2 * units, 2), range(half_chunks), range(half_chunks, nchunk)),
        (cross_y, range(1, 2 * units, 2), range(half_chunks, nchunk), range(half_chunks)),
    ):

        @pl.when(me == side)
        def _(side=side, relayed=relayed, mine=mine, theirs=theirs):
            for n in relayed:
                block_copy(far, n).wait_recv()
                relay_copy(n).start()
            for c in mine:
                first_hop(c).wait_recv()
                second_hop(c).start()
            for n in range(2 * units):
                block_copy(side, n).wait_recv()
            for c in theirs:
                third_hop(c).wait_recv()
            for n in relayed:
                relay_copy(n).wait_send()
            for c in mine:
                second_hop(c).wait_send()

    @pl.when(me == far)
    def _():
        for n in range(2 * units):
            relay_copy(n).wait_recv()
        for c in range(half_chunks):
            for half in (c, c + half_chunks):
                second_hop(half).wait_recv()
                third_hop(half).start()
        for c in range(nchunk):
            third_hop(c).wait_send()

    @pl.when(me != holder)
    def _():
        for copy in draft_copies(me):
            copy.wait_send()


def fused(holder, tab, old_keys, old_values, queries, draft_keys, draft_values):
    blocks = old_keys.shape[0]
    per_inst = blocks // 4
    requests, draft, width = queries.shape
    head_dim = old_keys.shape[3]
    rows = draft * (width // head_dim)
    block = old_keys.shape[1:]
    units = 4
    dma = pltpu.SemaphoreType.DMA
    any_space = pl.BlockSpec(memory_space=pl.ANY)
    bf = jnp.bfloat16
    return pl.pallas_call(
        functools.partial(fused_kernel, holder),
        out_shape=(
            jax.ShapeDtypeStruct((per_inst,) + block, bf),
            jax.ShapeDtypeStruct((per_inst,) + block, bf),
            jax.ShapeDtypeStruct(queries.shape, bf),
        ),
        in_specs=[pl.BlockSpec(memory_space=pltpu.SMEM)] + [any_space] * 5,
        out_specs=(any_space,) * 3,
        scratch_shapes=[
            pltpu.VMEM((blocks,) + block, bf),
            pltpu.VMEM((blocks,) + block, bf),
            pltpu.VMEM(queries.shape, bf),
            pltpu.VMEM((requests, draft, head_dim), bf),
            pltpu.VMEM((requests, draft, head_dim), bf),
            pltpu.VMEM((blocks,) + block, bf),
            pltpu.VMEM((blocks,) + block, bf),
            pltpu.VMEM((units, per_inst // units) + block, bf),
            pltpu.VMEM((blocks, draft, width), bf),
            pltpu.VMEM(queries.shape, bf),
            pltpu.VMEM((rows, head_dim), jnp.float32),
            pltpu.VMEM((rows, head_dim), jnp.float32),
            pltpu.VMEM((rows, head_dim), jnp.float32),
            dma((6,)),
            dma((2 * units,)),
            dma((2,)),
            dma((4, 2)),
            dma((4, 2 * units)),
            dma((4, 2 * units)),
            dma((2 * units,)),
            dma((2 * units,)),
            dma((8,)),
            dma((8,)),
            dma((8,)),
            dma((8,)),
        ],
        compiler_params=pltpu.CompilerParams(
            collective_id=1 + holder, has_side_effects=True, vmem_limit_bytes=60 * 1024 * 1024
        ),
    )(tab, old_keys, old_values, queries, draft_keys, draft_values)


def shards(old_keys, old_values, old_block, new_slot, lengths, queries, draft_keys, draft_values):
    insts = lax.axis_size("inst")
    plain = (
        insts == 4
        and old_block.shape[0] == new_slot.shape[0]
        and old_keys.shape[1] * old_keys.shape[2] == BLK
        and queries.shape[2] // old_keys.shape[3] == GROUP
        and lengths.shape[0] % 8 == 0
        and new_slot.shape[0] % BLK == 0
        and lengths.shape[0] <= new_slot.shape[0]
    )
    if not plain:
        return general_shards(
            old_keys, old_values, old_block, new_slot, lengths, queries, draft_keys, draft_values
        )
    tab = prepare(old_block, new_slot, lengths, insts)
    holder = tab[6, 0]
    return lax.switch(
        holder,
        [functools.partial(fused, h) for h in range(insts)],
        tab,
        old_keys,
        old_values,
        queries,
        draft_keys,
        draft_values,
    )


def solution(mesh):
    placed = (
        P("inst", "head", None, None),
        P("inst", "head", None, None),
        P("inst"),
        P(),
        P(),
        P(None, None, "head"),
        P("inst", None, None),
        P("inst", None, None),
    )
    return jax.shard_map(
        shards,
        mesh=mesh,
        in_specs=placed,
        out_specs=(
            P("inst", "head", None, None),
            P("inst", "head", None, None),
            P(None, None, "head"),
        ),
        check_vma=False,
    )
```

```python
import functools
import math

import jax
import jax.numpy as jnp
from jax import lax
from jax.experimental import pallas as pl
from jax.experimental.pallas import tpu as pltpu
from jax.sharding import PartitionSpec as P

GROUP = 8
BLK = 128
DRAFT = 16


masked = -1e30


def partner_2(block, axis, stride):
    count = lax.axis_size(axis)
    route = []
    for low in range(count):
        high = low | 1 << stride
        if high != low and high < count:
            route += [(low, high), (high, low)]
    return lax.ppermute(block, axis, route)


def join_partials(earlier, later):
    raised = jnp.maximum(earlier[0], later[0])
    keep_early = jnp.exp(earlier[0] - raised)
    keep_late = jnp.exp(later[0] - raised)
    totals = earlier[1] * keep_early + later[1] * keep_late
    weighted = earlier[2] * keep_early[..., None] + later[2] * keep_late[..., None]
    return (raised, totals, weighted)


def cache_partial(key_cache, value_cache, block_list, lengths, grouped, head_base):
    slot_count, entries, half_len, head_dim = key_cache.shape
    requests, qcount, _ = grouped.shape
    inv_root = 1.0 / math.sqrt(head_dim)
    counts = (lengths + BLK - 1) // BLK
    starts = jnp.cumsum(counts) - counts
    filled = block_list >= 0
    block_owner_list = (
        jnp.sum((starts[None, :] <= block_list[:, None]).astype(jnp.int32), axis=1) - 1
    )
    block_owner_list = jnp.clip(block_owner_list, 0, requests - 1)
    offset = block_list - starts[block_owner_list]
    halves = (head_base + jnp.arange(entries, dtype=jnp.int32)) % 2
    within = (halves[:, None] * half_len + jnp.arange(half_len, dtype=jnp.int32)[None, :]).reshape(
        entries * half_len
    )
    positions = offset[:, None] * BLK + within[None, :]
    usable = filled[:, None] & (positions < lengths[block_owner_list][:, None])
    stride = math.gcd(slot_count, 64)
    nsteps = slot_count // stride
    token_count = entries * half_len
    key_rows_all = key_cache.reshape(nsteps, stride, token_count, head_dim)
    value_rows_all = value_cache.reshape(nsteps, stride, token_count, head_dim)
    request_ids = jnp.arange(requests, dtype=jnp.int32)

    def advance(state_now, pieces):
        peaks, totals, weighted = state_now
        key_rows, value_rows, rows_owner, rows_filled, rows_usable = pieces
        picked = grouped[rows_owner]
        scores = (
            jnp.einsum("sqd,std->sqt", picked, key_rows, preferred_element_type=jnp.float32)
            * inv_root
        )
        scores = jnp.where(rows_usable[:, None, :], scores, masked)
        belongs = (rows_owner[:, None] == request_ids[None, :]) & rows_filled[:, None]
        slot_peaks = jnp.max(scores, axis=-1)
        block_peak = jnp.max(jnp.where(belongs[:, :, None], slot_peaks[:, None, :], masked), axis=0)
        raised = jnp.maximum(peaks, block_peak)
        weights = jnp.where(
            rows_usable[:, None, :], jnp.exp(scores - raised[rows_owner][:, :, None]), 0.0
        )
        belongs_f = belongs.astype(jnp.float32)
        row_sums = jnp.dot(
            belongs_f.T,
            jnp.sum(weights, axis=-1),
            precision=lax.Precision.HIGHEST,
            preferred_element_type=jnp.float32,
        )
        blended = jnp.einsum(
            "sqt,std->sqd",
            weights.astype(jnp.bfloat16),
            value_rows,
            preferred_element_type=jnp.float32,
        )
        gathered = jnp.einsum("sr,sqd->rqd", belongs_f, blended, precision=lax.Precision.HIGHEST)
        rescale = jnp.exp(peaks - raised)
        return (
            (raised, totals * rescale + row_sums, weighted * rescale[..., None] + gathered),
            None,
        )

    start_state = (
        jnp.full((requests, qcount), masked, jnp.float32),
        jnp.zeros((requests, qcount), jnp.float32),
        jnp.zeros((requests, qcount, head_dim), jnp.float32),
    )
    pieces = (
        key_rows_all,
        value_rows_all,
        block_owner_list.reshape(nsteps, stride),
        filled.reshape(nsteps, stride),
        usable.reshape(nsteps, stride, token_count),
    )
    return lax.scan(advance, start_state, pieces)[0]


def draft_partial(grouped, draft_keys, draft_values, current_replica, head_base):
    requests, qcount, head_dim = grouped.shape
    per_token = qcount // DRAFT
    rows_loc = draft_keys.shape[0]
    kv_head = head_base // 2
    own_keys = lax.dynamic_slice_in_dim(draft_keys, kv_head * head_dim, head_dim, 2)
    own_vals = lax.dynamic_slice_in_dim(draft_values, kv_head * head_dim, head_dim, 2)
    own_q = lax.dynamic_slice_in_dim(grouped, current_replica * rows_loc, rows_loc, 0).reshape(
        rows_loc, DRAFT, per_token, head_dim
    )
    inv_root = 1.0 / math.sqrt(head_dim)
    scores = (
        jnp.einsum("rigd,rjd->rigj", own_q, own_keys, preferred_element_type=jnp.float32) * inv_root
    )
    causal = jnp.arange(DRAFT)[None, :] <= jnp.arange(DRAFT)[:, None]
    causal_flat = jnp.broadcast_to(causal[:, None, :], (DRAFT, per_token, DRAFT)).reshape(
        qcount, DRAFT
    )
    scores = jnp.where(causal_flat, scores.reshape(rows_loc, qcount, DRAFT), masked)
    peaks = jnp.max(scores, axis=-1)
    weights = jnp.where(causal_flat, jnp.exp(scores - peaks[..., None]), 0.0)
    totals = jnp.sum(weights, axis=-1)
    weighted = jnp.einsum(
        "rqj,rjd->rqd", weights.astype(jnp.bfloat16), own_vals, preferred_element_type=jnp.float32
    )
    include = head_base % 2 == 0
    peaks = jnp.where(include, peaks, masked)
    totals = jnp.where(include, totals, 0.0)
    weighted = jnp.where(include, weighted, 0.0)
    first_row = current_replica * rows_loc
    full_peaks = lax.dynamic_update_slice_in_dim(
        jnp.full((requests, qcount), masked, jnp.float32), peaks, first_row, 0
    )
    full_totals = lax.dynamic_update_slice_in_dim(
        jnp.zeros((requests, qcount), jnp.float32), totals, first_row, 0
    )
    full_weighted = lax.dynamic_update_slice_in_dim(
        jnp.zeros((requests, qcount, head_dim), jnp.float32), weighted, first_row, 0
    )
    return (full_peaks, full_totals, full_weighted)


def general_shards(old_keys, old_values, old_block, new_slot, lengths, queries, draft_keys, draft_values):
    replica_count = lax.axis_size("inst")
    current_replica = lax.axis_index("inst")
    me_head = lax.axis_index("head")
    entries = old_keys.shape[1]
    head_dim = old_keys.shape[3]
    head_base = me_head * entries
    block_capacity = new_slot.shape[0]
    slots_per_replica = block_capacity // replica_count
    destination_replica = jnp.where(
        old_block >= 0, new_slot[jnp.clip(old_block, 0, block_capacity - 1)], block_capacity
    )
    trailing_tokens = old_keys.shape[1:]
    outgoing_keys = (
        jnp.zeros((block_capacity,) + trailing_tokens, old_keys.dtype)
        .at[destination_replica]
        .set(old_keys, mode="drop")
    )
    outgoing_values = (
        jnp.zeros((block_capacity,) + trailing_tokens, old_values.dtype)
        .at[destination_replica]
        .set(old_values, mode="drop")
    )
    outgoing_keys = outgoing_keys.reshape((replica_count, slots_per_replica) + trailing_tokens)
    outgoing_values = outgoing_values.reshape((replica_count, slots_per_replica) + trailing_tokens)
    inbox_k, inbox_v = (
        lax.all_to_all(outgoing_keys, "inst", split_axis=0, concat_axis=0, tiled=True),
        lax.all_to_all(outgoing_values, "inst", split_axis=0, concat_axis=0, tiled=True),
    )
    moved_keys = jnp.sum(inbox_k, axis=0)
    moved_values = jnp.sum(inbox_v, axis=0)
    local_heads = queries.shape[2] // head_dim
    requests = queries.shape[0]
    locally_present = (
        jnp.zeros((block_capacity,), jnp.int32)
        .at[new_slot]
        .set(jnp.arange(block_capacity, dtype=jnp.int32))
    )
    block_list = lax.dynamic_slice_in_dim(
        locally_present, current_replica * slots_per_replica, slots_per_replica
    )
    split_tokens = False
    if local_heads < GROUP:
        is_lower = me_head % 2 == 0
        partner = partner_2(queries, "head", 0)
        grouped = jnp.where(
            is_lower,
            jnp.concatenate([queries, partner], axis=2),
            jnp.concatenate([partner, queries], axis=2),
        )
        split_tokens = True
    else:
        grouped = queries
    qcount = grouped.shape[2] // head_dim
    grouped = grouped.reshape(requests, DRAFT * qcount, head_dim)
    cached = cache_partial(moved_keys, moved_values, block_list, lengths, grouped, head_base)
    drafted = draft_partial(grouped, draft_keys, draft_values, current_replica, head_base)
    peaks, totals, weighted = join_partials(cached, drafted)
    if split_tokens:
        peaks = peaks.reshape(requests, DRAFT, 2, local_heads)
        totals = totals.reshape(requests, DRAFT, 2, local_heads)
        weighted = weighted.reshape(requests, DRAFT, 2, local_heads, head_dim)
        is_first = me_head % 2 == 0
        own_peaks = jnp.where(is_first, peaks[:, :, 0], peaks[:, :, 1])
        own_totals = jnp.where(is_first, totals[:, :, 0], totals[:, :, 1])
        own_weighted = jnp.where(is_first, weighted[:, :, 0], weighted[:, :, 1])
        other_peaks = jnp.where(is_first, peaks[:, :, 1], peaks[:, :, 0])
        other_totals = jnp.where(is_first, totals[:, :, 1], totals[:, :, 0])
        other_weighted = jnp.where(is_first, weighted[:, :, 1], weighted[:, :, 0])
        received = partner_2((other_peaks, other_totals, other_weighted), "head", 0)
        peaks, totals, weighted = join_partials((own_peaks, own_totals, own_weighted), received)
    else:
        peaks = peaks.reshape(requests, DRAFT, local_heads)
        totals = totals.reshape(requests, DRAFT, local_heads)
        weighted = weighted.reshape(requests, DRAFT, local_heads, head_dim)
    top_score = lax.pmax(peaks, "inst")
    factor = jnp.exp(peaks - top_score)
    totals, weighted = lax.psum((totals * factor, weighted * factor[..., None]), "inst")
    attended = (
        (weighted / totals[..., None])
        .astype(jnp.bfloat16)
        .reshape(requests, DRAFT, local_heads * head_dim)
    )
    return (moved_keys, moved_values, attended)


UNROLL = 4
LIMIT = 60 * 1024 * 1024
SEND_SPLIT = 2


def prep_kernel(n, old_ref, slot_ref, len_ref, tab_ref, flag, got, padded, send_sem, recv_sem):
    me = lax.axis_index("inst")
    barrier = pltpu.get_barrier_semaphore()
    for step in range(1, n):
        pl.semaphore_signal(
            barrier,
            inc=1,
            device_id={"inst": lax.rem(me + step, n)},
            device_id_type=pl.DeviceIdType.MESH,
        )
    size = old_ref.shape[1]
    wide = (size, size)
    old = jnp.broadcast_to(old_ref[...], wide)
    filled = jnp.max(old[:8].astype(jnp.float32), axis=1, keepdims=True) >= 0.0
    flag[...] = jnp.broadcast_to(jnp.where(filled, me, 0), flag.shape)
    pl.semaphore_wait(barrier, n - 1)
    copies = []
    for step in range(1, n):
        copy = pltpu.make_async_remote_copy(
            src_ref=flag,
            dst_ref=got.at[step],
            send_sem=send_sem.at[step],
            recv_sem=recv_sem.at[step],
            device_id={"inst": lax.rem(me + step, n)},
            device_id_type=pl.DeviceIdType.MESH,
        )
        copy.start()
        copies.append(copy)

    r = lax.broadcasted_iota(jnp.int32, wide, 0)
    c = lax.broadcasted_iota(jnp.int32, wide, 1)

    def total(where, what, axis):
        return jnp.sum(jnp.where(where, what.astype(jnp.float32), 0.0), axis=axis, keepdims=True)

    old_t = old.T
    source = total(old_t == c, r, 0)
    placed = total(old_t == c, jnp.broadcast_to(slot_ref[...], wide), 1).astype(jnp.int32)
    placed = jnp.where(old_t >= 0, placed, -1)
    by_slot = total(placed == c, r, 0)
    padded[...] = jnp.zeros(padded.shape, jnp.int32)
    padded[0:1, : len_ref.shape[1]] = len_ref[...]
    length = jnp.broadcast_to(padded[0:1, :], wide)
    length_t = length.T
    counts = (length + (BLK - 1)) // BLK
    counts_t = (length_t + (BLK - 1)) // BLK
    ends = total(r <= c, counts_t, 0)
    ends_t = total(c <= r, counts, 1).astype(jnp.int32)
    starts_t = ends_t - counts_t
    inside = (starts_t <= c) & (c < ends_t)
    owner = total(inside, r, 0)
    live = jnp.minimum(total(inside, length_t - (c - starts_t) * BLK, 0), float(BLK))
    first = total(inside & (starts_t == c), jnp.ones(wide, jnp.int32), 0)
    rows = [source, by_slot, owner, live, first, ends - 1.0]
    for n_row, row in enumerate(rows):
        tab_ref[n_row : n_row + 1, :] = row.astype(jnp.int32)
    for copy in copies:
        copy.wait()
    holder = flag[0:1, :]
    for step in range(1, n):
        holder = holder + got[step, 0:1, :]
    tab_ref[6:7, :] = holder
    tab_ref[7:8, :] = holder


def prepare(old_block, new_slot, lengths, n):
    size = new_slot.shape[0]
    vmem = pl.BlockSpec(memory_space=pltpu.VMEM)
    return pl.pallas_call(
        functools.partial(prep_kernel, n),
        out_shape=jax.ShapeDtypeStruct((8, size), jnp.int32),
        in_specs=[vmem] * 3,
        out_specs=vmem,
        scratch_shapes=[
            pltpu.VMEM((8, size), jnp.int32),
            pltpu.VMEM((n, 8, size), jnp.int32),
            pltpu.VMEM((8, size), jnp.int32),
            pltpu.SemaphoreType.DMA((n,)),
            pltpu.SemaphoreType.DMA((n,)),
        ],
        compiler_params=pltpu.CompilerParams(collective_id=0, has_side_effects=True),
    )(old_block.reshape(1, size), new_slot.reshape(1, size), lengths.reshape(1, lengths.shape[0]))


def fused_kernel(
    holder,
    tab,
    keys_hbm,
    values_hbm,
    queries_hbm,
    dkeys_hbm,
    dvals_hbm,
    mk_out,
    mv_out,
    att_out,
    kbuf,
    vbuf,
    qbuf,
    dk,
    dv,
    send_k,
    send_v,
    relay,
    per_block,
    att,
    m_ref,
    l_ref,
    acc_ref,
    load_sem,
    keep_sem,
    draft_send,
    draft_recv,
    blk_send,
    blk_recv,
    fwd_send,
    fwd_recv,
    att_send,
    att_recv,
    pass_send,
    pass_recv,
):
    me = lax.axis_index("inst")
    head = lax.axis_index("head")
    mesh_id = pl.DeviceIdType.MESH
    cross_x, cross_y, far = holder ^ 1, holder ^ 2, holder ^ 3
    insts = 4
    blocks = kbuf.shape[0]
    per_inst = blocks // insts
    head_dim = kbuf.shape[3]
    requests = qbuf.shape[0]
    rows_loc = requests // insts
    local_heads = qbuf.shape[2] // head_dim
    units = 4
    unit = per_inst // units
    nchunk = 8
    chunk = requests // nchunk
    half_chunks = nchunk // 2

    barrier = pltpu.get_barrier_semaphore()
    for step in range(1, insts):
        pl.semaphore_signal(
            barrier, inc=1, device_id={"inst": lax.rem(me + step, insts)}, device_id_type=mesh_id
        )

    lanes = pl.ds(pl.multiple_of(head * head_dim, head_dim), head_dim)

    loads = [
        pltpu.make_async_copy(src, dst, load_sem.at[n])
        for n, (src, dst) in enumerate(
            (
                (keys_hbm, kbuf),
                (values_hbm, vbuf),
                (queries_hbm, qbuf),
                (dkeys_hbm.at[:, :, lanes], dk.at[pl.ds(holder * rows_loc, rows_loc)]),
                (dvals_hbm.at[:, :, lanes], dv.at[pl.ds(holder * rows_loc, rows_loc)]),
            )
        )
    ]

    @pl.when(me == holder)
    def _():
        loads[0].start()

    pl.semaphore_wait(barrier, insts - 1)

    def draft_copies(origin):
        rows = pl.ds(origin * rows_loc, rows_loc)
        return [
            pltpu.make_async_remote_copy(
                src_ref=src.at[:, :, lanes],
                dst_ref=dst.at[rows],
                send_sem=draft_send.at[n],
                recv_sem=draft_recv.at[origin, n],
                device_id={"inst": holder},
                device_id_type=mesh_id,
            )
            for n, (src, dst) in enumerate(((dkeys_hbm, dk), (dvals_hbm, dv)))
        ]

    def out_of(n):
        return (mk_out, mv_out)[n // units].at[pl.ds((n % units) * unit, unit)]

    def staged(inst, n):
        return (send_k, send_v)[n // units].at[pl.ds(inst * per_inst + (n % units) * unit, unit)]

    def block_copy(inst, n):
        if inst == far:
            to = cross_x if n % 2 == 0 else cross_y
            dst = relay.at[n // 2]
        else:
            to = inst
            dst = out_of(n)
        return pltpu.make_async_remote_copy(
            src_ref=staged(inst, n),
            dst_ref=dst,
            send_sem=blk_send.at[inst, n],
            recv_sem=blk_recv.at[inst, n],
            device_id={"inst": to},
            device_id_type=mesh_id,
        )

    def relay_copy(n):
        return pltpu.make_async_remote_copy(
            src_ref=relay.at[n // 2],
            dst_ref=out_of(n),
            send_sem=fwd_send.at[n],
            recv_sem=fwd_recv.at[n],
            device_id={"inst": far},
            device_id_type=mesh_id,
        )

    def att_copy(src, c, to, send, recv):
        rows = pl.ds(c * chunk, chunk)
        return pltpu.make_async_remote_copy(
            src_ref=src.at[rows],
            dst_ref=att_out.at[rows],
            send_sem=send.at[c],
            recv_sem=recv.at[c],
            device_id={"inst": to},
            device_id_type=mesh_id,
        )

    def first_hop(c):
        return att_copy(att, c, cross_x if c < half_chunks else cross_y, att_send, att_recv)

    def second_hop(c):
        return att_copy(att_out, c, far, pass_send, pass_recv)

    def third_hop(c):
        return att_copy(
            att_out, c, cross_y if c < half_chunks else cross_x, att_send, att_recv
        )

    @pl.when(me == holder)
    def _():
        def fill(inst, n):
            src, dst = ((kbuf, send_k), (vbuf, send_v))[n // units]

            def one(i, _):
                slot = inst * per_inst + (n % units) * unit + i
                dst[slot] = src[tab[1, slot]]
                return 0

            lax.fori_loop(0, unit, one, 0, unroll=4)

        def stage(pairs):
            for at, pair in enumerate(pairs):
                fill(*pair)
                if at >= 2:
                    block_copy(*pairs[at - 2]).start()
            for pair in pairs[-2:]:
                block_copy(*pair).start()

        loads[0].wait()
        loads[1].start()
        early = [(inst, n) for n in range(SEND_SPLIT) for inst in (cross_x, cross_y)]
        stage([(far, n) for n in range(units)] + early)
        loads[1].wait()
        for load in loads[2:]:
            load.start()
        stage([(far, n) for n in range(units, 2 * units)])
        for n in range(SEND_SPLIT, 2 * units):
            fill(cross_x, n)
            fill(cross_y, n)
        for n in range(2 * units):
            fill(holder, n)

        for load in loads[2:]:
            load.wait()
        for origin in (cross_x, cross_y, far):
            for copy in draft_copies(origin):
                copy.wait_recv()

        inv_root = 1.0 / math.sqrt(head_dim)
        rows = DRAFT * local_heads
        cols = BLK + DRAFT
        col = lax.broadcasted_iota(jnp.int32, (rows, cols), 1)
        row = lax.broadcasted_iota(jnp.int32, (rows, cols), 0)
        causal = (col >= BLK) & (col - BLK <= row % DRAFT)
        causal_i = causal.astype(jnp.int32)
        m_ref[...] = jnp.full(m_ref.shape, masked, jnp.float32)
        l_ref[...] = jnp.zeros(l_ref.shape, jnp.float32)
        acc_ref[...] = jnp.zeros(acc_ref.shape, jnp.float32)

        def attend(step, _):
            parts = []
            for u in range(UNROLL):
                g = step * UNROLL + u
                spot, owner, live, first = tab[0, g], tab[2, g], tab[3, g], tab[4, g]
                q = qbuf[owner]
                q = jnp.concatenate(
                    [q[:, j * head_dim : (j + 1) * head_dim] for j in range(local_heads)], axis=0
                )
                k = jnp.concatenate([kbuf[spot].reshape(BLK, head_dim), dk[owner]], axis=0)
                v = jnp.concatenate([vbuf[spot].reshape(BLK, head_dim), dv[owner]], axis=0)
                s = (
                    lax.dot_general(
                        q, k, (((1,), (1,)), ((), ())), preferred_element_type=jnp.float32
                    )
                    * inv_root
                )
                usable = (col < live) | (causal_i * first > 0)
                s = jnp.where(usable, s, masked)
                m = jnp.max(s, axis=1, keepdims=True)
                p = jnp.exp(s - m)
                l = jnp.sum(p, axis=1, keepdims=True)
                acc = jnp.dot(p.astype(jnp.bfloat16), v, preferred_element_type=jnp.float32)
                parts.append((g, first, m, l, acc))
            m_run, l_run, acc_run = m_ref[...], l_ref[...], acc_ref[...]
            for g, first, m, l, acc in parts:
                m_run = jnp.where(first > 0, masked, m_run)
                raised = jnp.maximum(m_run, m)
                old = jnp.exp(m_run - raised)
                new = jnp.exp(m - raised)
                m_run = raised
                l_run = l_run * old + l * new
                acc_run = acc_run * old + acc * new
                out = (acc_run / l_run).astype(jnp.bfloat16)
                for j in range(local_heads):
                    per_block[g, :, j * head_dim : (j + 1) * head_dim] = out[
                        j * DRAFT : (j + 1) * DRAFT
                    ]
            m_ref[...], l_ref[...], acc_ref[...] = m_run, l_run, acc_run
            return 0

        lax.fori_loop(0, blocks // UNROLL, attend, 0)

        def pick(r, _):
            att[r] = per_block[tab[5, r]]
            return 0

        lax.fori_loop(0, requests, pick, 0)
        keeps = [
            pltpu.make_async_copy(staged(holder, n), out_of(n), keep_sem.at[n])
            for n in range(2 * units)
        ]
        for keep in keeps:
            keep.start()
        for c in range(half_chunks):
            first_hop(c).start()
            first_hop(c + half_chunks).start()
        for n in range(SEND_SPLIT, 2 * units):
            block_copy(cross_x, n).start()
            block_copy(cross_y, n).start()
        own = pltpu.make_async_copy(att, att_out, load_sem.at[5])
        own.start()
        for keep in keeps:
            keep.wait()
        own.wait()
        for n in range(2 * units):
            for inst in (far, cross_x, cross_y):
                block_copy(inst, n).wait_send()
        for c in range(nchunk):
            first_hop(c).wait_send()

    @pl.when(me != holder)
    def _():
        for copy in draft_copies(me):
            copy.start()

    for side, relayed, mine, theirs in (
        (cross_x, range(0, 2 * units, 2), range(half_chunks), range(half_chunks, nchunk)),
        (cross_y, range(1, 2 * units, 2), range(half_chunks, nchunk), range(half_chunks)),
    ):

        @pl.when(me == side)
        def _(side=side, relayed=relayed, mine=mine, theirs=theirs):
            for n in relayed:
                block_copy(far, n).wait_recv()
                relay_copy(n).start()
            for c in mine:
                first_hop(c).wait_recv()
                second_hop(c).start()
            for n in range(2 * units):
                block_copy(side, n).wait_recv()
            for c in theirs:
                third_hop(c).wait_recv()
            for n in relayed:
                relay_copy(n).wait_send()
            for c in mine:
                second_hop(c).wait_send()

    @pl.when(me == far)
    def _():
        for n in range(2 * units):
            relay_copy(n).wait_recv()
        for c in range(half_chunks):
            for half in (c, c + half_chunks):
                second_hop(half).wait_recv()
                third_hop(half).start()
        for c in range(nchunk):
            third_hop(c).wait_send()

    @pl.when(me != holder)
    def _():
        for copy in draft_copies(me):
            copy.wait_send()


def fused(holder, tab, old_keys, old_values, queries, draft_keys, draft_values):
    blocks = old_keys.shape[0]
    per_inst = blocks // 4
    requests, draft, width = queries.shape
    head_dim = old_keys.shape[3]
    rows = draft * (width // head_dim)
    block = old_keys.shape[1:]
    units = 4
    dma = pltpu.SemaphoreType.DMA
    any_space = pl.BlockSpec(memory_space=pl.ANY)
    bf = jnp.bfloat16
    return pl.pallas_call(
        functools.partial(fused_kernel, holder),
        out_shape=(
            jax.ShapeDtypeStruct((per_inst,) + block, bf),
            jax.ShapeDtypeStruct((per_inst,) + block, bf),
            jax.ShapeDtypeStruct(queries.shape, bf),
        ),
        in_specs=[pl.BlockSpec(memory_space=pltpu.SMEM)] + [any_space] * 5,
        out_specs=(any_space,) * 3,
        scratch_shapes=[
            pltpu.VMEM((blocks,) + block, bf),
            pltpu.VMEM((blocks,) + block, bf),
            pltpu.VMEM(queries.shape, bf),
            pltpu.VMEM((requests, draft, head_dim), bf),
            pltpu.VMEM((requests, draft, head_dim), bf),
            pltpu.VMEM((blocks,) + block, bf),
            pltpu.VMEM((blocks,) + block, bf),
            pltpu.VMEM((units, per_inst // units) + block, bf),
            pltpu.VMEM((blocks, draft, width), bf),
            pltpu.VMEM(queries.shape, bf),
            pltpu.VMEM((rows, head_dim), jnp.float32),
            pltpu.VMEM((rows, head_dim), jnp.float32),
            pltpu.VMEM((rows, head_dim), jnp.float32),
            dma((6,)),
            dma((2 * units,)),
            dma((2,)),
            dma((4, 2)),
            dma((4, 2 * units)),
            dma((4, 2 * units)),
            dma((2 * units,)),
            dma((2 * units,)),
            dma((8,)),
            dma((8,)),
            dma((8,)),
            dma((8,)),
        ],
        compiler_params=pltpu.CompilerParams(
            collective_id=1 + holder, has_side_effects=True, vmem_limit_bytes=LIMIT
        ),
    )(tab, old_keys, old_values, queries, draft_keys, draft_values)


def shards(old_keys, old_values, old_block, new_slot, lengths, queries, draft_keys, draft_values):
    insts = lax.axis_size("inst")
    plain = (
        insts == 4
        and old_block.shape[0] == new_slot.shape[0]
        and old_keys.shape[1] * old_keys.shape[2] == BLK
        and queries.shape[2] // old_keys.shape[3] == GROUP
        and lengths.shape[0] % 8 == 0
        and new_slot.shape[0] % BLK == 0
        and lengths.shape[0] <= new_slot.shape[0]
    )
    if not plain:
        return general_shards(
            old_keys, old_values, old_block, new_slot, lengths, queries, draft_keys, draft_values
        )
    tab = prepare(old_block, new_slot, lengths, insts)
    holder = tab[6, 0]
    return lax.switch(
        holder,
        [functools.partial(fused, h) for h in range(insts)],
        tab,
        old_keys,
        old_values,
        queries,
        draft_keys,
        draft_values,
    )


def solution(mesh):
    placed = (
        P("inst", "head", None, None),
        P("inst", "head", None, None),
        P("inst"),
        P(),
        P(),
        P(None, None, "head"),
        P("inst", None, None),
        P("inst", None, None),
    )
    return jax.shard_map(
        shards,
        mesh=mesh,
        in_specs=placed,
        out_specs=(
            P("inst", "head", None, None),
            P("inst", "head", None, None),
            P(None, None, "head"),
        ),
        check_vma=False,
    )
```
